256 devices in a mesh: worker: 16 (over x_lo, y, core), mp: 16 (over x_hi, z).
Axes of the slice: x: 4 (x_hi: 2, x_lo: 2; x = x_hi * 2 + x_lo), y: 4, z: 8, core: 2. Of those that a mesh axis runs over, the one named last changes fastest.
Arguments:
- grad: bfloat16 [16, 2048, 14336], P('worker', 'mp'), may hold values from -24 to 24
Outputs:
- median: bfloat16 [2048, 14336], P('mp')
- trimmed: bfloat16 [2048, 14336], P('mp')
The draws below stay inside these ranges and needn't reach their ends.
All inputs are finite; a program needn't handle non-finite values.
Results may differ from the reference program's by a relative error of at most 0.0048.
Values may be sent and summed in bfloat16 or wider, within the bound.
No kernel may reach another device: no remote copies, remote signals or barrier semaphores. Data moves between devices by JAX's collectives and lax.ppermute only.
A program may use at most 64 MiB of HBM per device.

```python
import math
import jax
import jax.numpy as jnp
import numpy as np
from jax import lax

FF = 14336
ROWS_DEV = 128
ROWS = 2048
WORKERS = 16


def draw_grad(key, part):
    first_key, second_key, third_key = jax.random.split(key, 3)
    row_scales = jnp.exp(jax.random.uniform(second_key, (WORKERS, ROWS, 1), jnp.float32, math.log(0.25), math.log(4.0)))
    values = jnp.clip(jax.random.normal(first_key, (WORKERS, ROWS, FF), jnp.float32), -6.0, 6.0)
    return jnp.clip(values * row_scales, -24.0, 24.0).astype(jnp.bfloat16)


def setup_inputs(seed: int = 0) -> dict:
    key_list = jax.random.split(jax.random.key(seed), 2)
    grad = draw_grad(jax.random.fold_in(key_list[1], 71), 0)
    return dict(grad=grad)


def sort_copies(stacked):
    copies = stacked.shape[0]
    rest = stacked.shape[1:]
    positions = np.arange(copies)
    span_size = 2
    while span_size <= copies:
        step_size = span_size // 2
        while step_size >= 1:
            grouped = stacked.reshape((copies // (2 * step_size), 2, step_size) + rest)
            partner = jnp.flip(grouped, 1).reshape(stacked.shape)
            lowest = jnp.minimum(stacked, partner)
            highest = jnp.maximum(stacked, partner)
            keep_table = (positions & step_size == 0) == (positions & span_size == 0)
            keep_mask = jnp.asarray(keep_table).reshape((copies,) + (1,) * len(rest))
            stacked = jnp.where(keep_mask, lowest, highest)
            step_size = step_size // 2
        span_size = span_size * 2
    return stacked

def summarize(stacked):
    ordered = sort_copies(stacked)
    copies = ordered.shape[0]
    middle = copies // 2
    trim_count = copies // 4
    median = ((ordered[middle - 1].astype(jnp.float32) + ordered[middle].astype(jnp.float32)) * 0.5).astype(jnp.bfloat16)
    kept = lax.optimization_barrier(jnp.sum(ordered[trim_count:copies - trim_count].astype(jnp.float32), axis=0)) / (copies - 2 * trim_count)
    return (median, kept.astype(jnp.bfloat16))

def reference(grad):

    def worker_power(copy_rows):
        return jnp.sum(jnp.square(copy_rows.astype(jnp.float32)))
    power = lax.map(worker_power, grad)
    factor = lax.rsqrt(power / (ROWS * FF) + 0.25)
    block_rows = ROWS_DEV
    blocks = ROWS // block_rows

    def one_block(block_index):
        start = (block_index * block_rows).astype(jnp.int32)
        piece = lax.dynamic_slice_in_dim(grad, start, block_rows, 1)
        scaled = (piece.astype(jnp.float32) * factor[:, None, None]).astype(jnp.bfloat16)
        return summarize(scaled)
    median, trimmed = lax.map(one_block, jnp.arange(blocks, dtype=jnp.int32))
    return (median.reshape(ROWS, FF), trimmed.reshape(ROWS, FF))
```

```python
import functools

import jax
import jax.numpy as jnp
from jax import lax
from jax.experimental import pallas as pl
from jax.experimental.pallas import tpu as pltpu
from jax.sharding import PartitionSpec as P


SORT8 = (
    (0, 1), (2, 3), (4, 5), (6, 7),
    (0, 2), (1, 3), (4, 6), (5, 7),
    (1, 2), (5, 6),
    (0, 4), (1, 5), (2, 6), (3, 7),
    (2, 4), (3, 5),
    (1, 2), (3, 4), (5, 6),
)


def sort8(values):
    values = list(values)
    for low, high in SORT8:
        a, b = values[low], values[high]
        values[low], values[high] = jnp.minimum(a, b), jnp.maximum(a, b)
    return values


def middle(values):
    left, right = sort8(values[:8]), sort8(values[8:])
    lower = [jnp.minimum(left[i], right[7 - i]) for i in range(8)]
    upper = [jnp.maximum(left[i], right[7 - i]) for i in range(8)]
    lower = [jnp.maximum(lower[i], lower[i + 4]) for i in range(4)]
    upper = [jnp.minimum(upper[i], upper[i + 4]) for i in range(4)]
    seventh = jnp.maximum(jnp.maximum(lower[0], lower[1]), jnp.maximum(lower[2], lower[3]))
    eighth = jnp.minimum(jnp.minimum(upper[0], upper[1]), jnp.minimum(upper[2], upper[3]))
    kept = [v.astype(jnp.float32) for v in lower + upper]
    while len(kept) > 1:
        kept = [a + b for a, b in zip(kept[::2], kept[1::2])]
    return seventh.astype(jnp.float32), eighth.astype(jnp.float32), kept[0]


def aggregate_kernel(factor_ref, copies_ref, median_ref, trimmed_ref, *, lanes):
    workers, rows, columns = copies_ref.shape

    def step(i, carry):
        at = pl.ds(pl.multiple_of(i * lanes, lanes), lanes)
        scaled = [
            (copies_ref[w, :, at].astype(jnp.float32) * factor_ref[w]).astype(jnp.bfloat16)
            for w in range(workers)
        ]
        seventh, eighth, total = middle(scaled)
        median_ref[:, at] = ((seventh + eighth) * 0.5).astype(jnp.bfloat16)
        trimmed_ref[:, at] = (total * 0.125).astype(jnp.bfloat16)
        return carry

    lax.fori_loop(0, columns // lanes, step, 0)


def aggregate(copies, factors):
    workers, rows, columns = copies.shape
    block = columns // 7
    out = jax.ShapeDtypeStruct((rows, columns), jnp.bfloat16)
    return pl.pallas_call(
        functools.partial(aggregate_kernel, lanes=256),
        grid=(columns // block,),
        in_specs=[
            pl.BlockSpec(memory_space=pltpu.SMEM),
            pl.BlockSpec((workers, rows, block), lambda i: (0, 0, i)),
        ],
        out_specs=[pl.BlockSpec((rows, block), lambda i: (0, i))] * 2,
        out_shape=[out, out],
        cost_estimate=pl.CostEstimate(
            flops=workers * rows * columns * 8, bytes_accessed=workers * rows * columns * 2, transcendentals=0
        ),
        name="aggregate",
    )(factors, copies)


def shards(grad):
    _, rows, columns = grad.shape
    workers = lax.axis_size("worker")
    pieces = grad.reshape(workers, rows // workers, columns)
    copies = lax.all_to_all(pieces, "worker", 0, 0, tiled=True)
    power = lax.psum(jnp.sum(jnp.square(grad.astype(jnp.float32))), "mp")
    factor = lax.rsqrt(power / (rows * lax.axis_size("mp") * columns) + 0.25)
    factors = lax.all_gather(factor, "worker")
    median, trimmed = aggregate(copies, factors)
    return tuple(lax.all_gather(a, "worker", axis=0, tiled=True) for a in (median, trimmed))


def solution(mesh):
    return jax.shard_map(
        shards,
        mesh=mesh,
        in_specs=(P("worker", "mp", None),),
        out_specs=(P("mp", None), P("mp", None)),
        check_vma=False,
    )
```
